32 devices in a mesh: parts: 4 (over y, z), data: 8 (over x, core).
Axes of the slice: x: 4, y: 2, z: 2, core: 2. Of those that a mesh axis runs over, the one named last changes fastest.
The devices are a block of a 4x4x8 slice.
Arguments:
- features: bfloat16 [16384, 1536], P('data')
- labels: int32 [16384], P('data')
- theta_start: float32 [1536, 8], P(None, 'parts'), parts along dimension 1
- momentum_start: float32 [1536, 8], P(None, 'parts'), parts along dimension 1
Outputs:
- output 1: float32 [1536, 8], P(None, 'parts'), parts along dimension 1
- output 2: float32 [1536, 8], P(None, 'parts'), parts along dimension 1
- output 3: float32 [8], P('parts'), parts along dimension 0
There are 4 independent parts. The reference program is written for one: setup_inputs(seed, part) draws one part's arguments, and reference() takes and returns one part's arrays. A program takes and returns all parts, laid end to end along the dimension named above; an argument that names none is the same for every part.
All inputs are finite; a program needn't handle non-finite values.
Results may differ from the reference program's by a relative error of at most 0.00262983.
Values are sent between devices in bfloat16 or wider.
A program may use at most 768 MiB of HBM per device.

```python
import math
import jax
import jax.numpy as jnp
from jax import lax

D = 1536
CHAINS = 2
ROWS_DEV = 2048
DATA = 8
LEAPFROG = 32
ROWS = ROWS_DEV * DATA


def setup_inputs(seed: int = 0, part: int = 0) -> dict:
    base_key = jax.random.key(seed)
    key_feat, key_label, key_sign = jax.random.split(base_key, 3)
    part_key = jax.random.fold_in(jax.random.key(seed + 1), part)
    key_pos, key_mom = jax.random.split(part_key)
    shard_ids = jnp.arange(DATA, dtype=jnp.int32)
    label_blocks = jax.random.randint(key_label, (DATA, ROWS_DEV), 0, 2, dtype=jnp.int32)
    col_sign = jax.random.rademacher(key_sign, (D,), dtype=jnp.float32)
    col_owner = jnp.arange(D, dtype=jnp.int32) % DATA
    amp_base = math.sqrt(0.5 / D)
    amp_boost = math.sqrt((0.5 + 1.5 * DATA) / D)
    class_gap = 1.0 / math.sqrt(D)

    def draw_block(shard_args):
        shard, block_labels = shard_args
        noise = jax.random.normal(jax.random.fold_in(key_feat, shard), (ROWS_DEV, D), jnp.float32)
        signed = (2.0 * block_labels.astype(jnp.float32) - 1.0)[:, None] * col_sign[None, :] * class_gap
        col_amp = jnp.where(col_owner == shard, amp_boost, amp_base)
        return ((noise + signed) * col_amp[None, :]).astype(jnp.bfloat16)

    features = lax.map(draw_block, (shard_ids, label_blocks)).reshape(ROWS, D)
    theta_start = 0.5 * jax.random.normal(key_pos, (D, CHAINS), jnp.float32)
    momentum_start = jax.random.normal(key_mom, (D, CHAINS), jnp.float32)
    return {'features': features, 'labels': label_blocks.reshape(ROWS), 'theta_start': theta_start, 'momentum_start': momentum_start}


def reference(features, labels, theta_start, momentum_start):
    prior_var = 1.0
    step_size = 0.3 * math.sqrt(D / ROWS)
    label_col = labels.astype(jnp.float32)[:, None]

    def grad_fn(position):
        logits = jnp.dot(features, position.astype(jnp.bfloat16), preferred_element_type=jnp.float32)
        residual = (label_col - jax.nn.sigmoid(logits)).astype(jnp.bfloat16)
        lik_grad = lax.dot_general(features, residual, (((0,), (0,)), ((), ())), preferred_element_type=jnp.float32)
        return lik_grad - position / prior_var, logits

    grad_val, _ = grad_fn(theta_start)
    momentum = momentum_start + 0.5 * step_size * grad_val

    def loop_body(carry, unused):
        position, moment_cur = carry
        position = position + step_size * moment_cur
        grad_cur, _ = grad_fn(position)
        return (position, moment_cur + step_size * grad_cur), None

    (position, momentum), _ = lax.scan(loop_body, (theta_start, momentum), None, length=LEAPFROG - 1)
    position = position + step_size * momentum
    grad_val, logits = grad_fn(position)
    momentum = momentum + 0.5 * step_size * grad_val
    potential = jnp.sum(jax.nn.softplus(logits) - label_col * logits, axis=0) + jnp.sum(position * position, axis=0) / (2.0 * prior_var)
    energy = potential + 0.5 * jnp.sum(momentum * momentum, axis=0)
    return position, momentum, energy
```

```python
import functools
import math
import jax
import jax.numpy as jnp
from jax import lax
from jax.experimental import pallas as pl
from jax.experimental.pallas import tpu as pltpu
from jax.sharding import PartitionSpec as P

LEAPFROG = 32
PRIOR_VAR = 1.0
STEP_COEF = 0.3
CHUNK = 512
TILE = 256


def trajectory(n, step_size, feat_hbm, label_ref, theta0_ref, mom0_ref,
               theta_out, mom_out, energy_out,
               feat, feat_t, logits_ref, theta_ref, mom_ref, buf, ebuf,
               load_sem, send_sem, recv_sem, esend_sem, erecv_sem):
    rows, dim = feat.shape
    chains = theta0_ref.shape[0]
    chunks = dim // CHUNK
    row_tiles = rows // TILE
    me = lax.axis_index('data')
    chip, core = me // 2, me % 2
    chips = n // 2
    hops = sorted(range(chips), key=lambda d: -min(d, chips - d))
    peers = [lax.rem(chip + d, chips) * 2 + (lax.rem(core + c, 2)) for d in hops for c in (0, 1) if (d, c) != (0, 0)]

    loads = []
    for t in range(row_tiles):
        copy = pltpu.make_async_copy(feat_hbm.at[pl.ds(t * TILE, TILE), :], feat.at[pl.ds(t * TILE, TILE), :], load_sem.at[t])
        copy.start()
        loads.append(copy)

    barrier = pltpu.get_barrier_semaphore()
    for peer in peers:
        pl.semaphore_signal(barrier, inc=1, device_id={'data': peer}, device_id_type=pl.DeviceIdType.MESH)

    theta_ref[...] = theta0_ref[...]
    mom_ref[...] = mom0_ref[...]

    def lhs(v):
        return jnp.concatenate([v, jnp.zeros((8 - chains, v.shape[1]), jnp.float32)], axis=0).astype(jnp.bfloat16)

    theta16 = lhs(theta0_ref[...])
    for t in range(row_tiles):
        loads[t].wait()
        for c in range(dim // TILE):
            feat_t[c * TILE:(c + 1) * TILE, t * TILE:(t + 1) * TILE] = feat[t * TILE:(t + 1) * TILE, c * TILE:(c + 1) * TILE].T
        logits_ref[:, t * TILE:(t + 1) * TILE] = jnp.dot(theta16, feat_t[:, t * TILE:(t + 1) * TILE], preferred_element_type=jnp.float32)

    pl.semaphore_wait(barrier, n - 1)

    def evaluate(step, last):
        par = lax.rem(step, 2)
        label_row = label_ref[...].astype(jnp.float32)
        logits = logits_ref[...]
        if last:
            z = logits[:chains]
            terms = jnp.maximum(z, 0.0) + jnp.log1p(jnp.exp(-jnp.abs(z))) - label_row * z
            part = terms[:, 0:128]
            for j in range(1, rows // 128):
                part = part + terms[:, j * 128:(j + 1) * 128]
            ebuf[me] = part
            for i, peer in enumerate(peers):
                pltpu.make_async_remote_copy(src_ref=ebuf.at[me], dst_ref=ebuf.at[me], send_sem=esend_sem, recv_sem=erecv_sem,
                                             device_id={'data': peer}, device_id_type=pl.DeviceIdType.MESH).start()
        residual = (label_row - jax.nn.sigmoid(logits)).astype(jnp.bfloat16)
        for c in range(chunks):
            cols = pl.ds(c * CHUNK, CHUNK)
            part_grad = jnp.dot(residual, feat[:, cols], preferred_element_type=jnp.float32)
            buf[par, c, me] = part_grad[:chains]
            for peer in peers:
                pltpu.make_async_remote_copy(src_ref=buf.at[par, c, me], dst_ref=buf.at[par, c, me],
                                             send_sem=send_sem.at[par, c], recv_sem=recv_sem.at[par, c],
                                             device_id={'data': peer}, device_id_type=pl.DeviceIdType.MESH).start()
        half = jnp.where(step == 0, 0.5 * step_size, step_size) if not last else 0.5 * step_size
        for c in range(chunks):
            cols = pl.ds(c * CHUNK, CHUNK)
            others = buf.at[par, c, pl.ds(0, n - 1)]
            pltpu.make_async_copy(others, others, recv_sem.at[par, c]).wait()
            grad = buf[par, c, 0]
            for k in range(1, n):
                grad = grad + buf[par, c, k]
            theta = theta_ref[:, cols]
            mom = mom_ref[:, cols] + half * (grad - theta / PRIOR_VAR)
            mom_ref[:, cols] = mom
            if not last:
                theta = theta + step_size * mom
                theta_ref[:, cols] = theta
                part = jnp.dot(lhs(theta), feat_t[cols, :], preferred_element_type=jnp.float32)
                if c == 0:
                    logits_ref[...] = part
                else:
                    logits_ref[...] = logits_ref[...] + part
        for c in range(chunks):
            others = buf.at[par, c, pl.ds(0, n - 1)]
            pltpu.make_async_copy(others, others, send_sem.at[par, c]).wait()

    def body(step, carry):
        evaluate(step, False)
        return carry

    lax.fori_loop(0, LEAPFROG, body, 0)
    evaluate(LEAPFROG, True)

    others = ebuf.at[pl.ds(0, n - 1)]
    pltpu.make_async_copy(others, others, erecv_sem).wait()
    pltpu.make_async_copy(others, others, esend_sem).wait()
    row_sum = ebuf[0]
    for k in range(1, n):
        row_sum = row_sum + ebuf[k]
    theta, mom = theta_ref[...], mom_ref[...]
    theta_out[...] = theta
    mom_out[...] = mom
    energy = (jnp.sum(row_sum, axis=1, keepdims=True) + jnp.sum(theta * theta, axis=1, keepdims=True) / (2.0 * PRIOR_VAR)
              + 0.5 * jnp.sum(mom * mom, axis=1, keepdims=True))
    energy_out[...] = jnp.broadcast_to(energy, energy_out.shape)


def solution(mesh):
    n = mesh.shape['data']

    def local_run(feat_loc, label_loc, theta_start, momentum_start):
        rows, dim = feat_loc.shape
        chains = theta_start.shape[1]
        chunks = dim // CHUNK
        step_size = STEP_COEF * math.sqrt(dim / (rows * n))
        vmem = pl.BlockSpec(memory_space=pltpu.VMEM)
        theta, mom, energy = pl.pallas_call(
            functools.partial(trajectory, n, step_size),
            out_shape=(jax.ShapeDtypeStruct((chains, dim), jnp.float32), jax.ShapeDtypeStruct((chains, dim), jnp.float32),
                       jax.ShapeDtypeStruct((chains, 128), jnp.float32)),
            in_specs=[pl.BlockSpec(memory_space=pl.ANY), vmem, vmem, vmem],
            out_specs=(vmem, vmem, vmem),
            scratch_shapes=[
                pltpu.VMEM((rows, dim), jnp.bfloat16),
                pltpu.VMEM((dim, rows), jnp.bfloat16),
                pltpu.VMEM((8, rows), jnp.float32),
                pltpu.VMEM((chains, dim), jnp.float32),
                pltpu.VMEM((chains, dim), jnp.float32),
                pltpu.VMEM((2, chunks, n, chains, CHUNK), jnp.float32),
                pltpu.VMEM((n, chains, 128), jnp.float32),
                pltpu.SemaphoreType.DMA((rows // TILE,)),
                pltpu.SemaphoreType.DMA((2, chunks)),
                pltpu.SemaphoreType.DMA((2, chunks)),
                pltpu.SemaphoreType.DMA,
                pltpu.SemaphoreType.DMA,
            ],
            compiler_params=pltpu.CompilerParams(collective_id=0, has_side_effects=True, vmem_limit_bytes=48 * 1024 * 1024),
            name='trajectory',
        )(feat_loc, label_loc[None, :], theta_start.T, momentum_start.T)
        return theta.T, mom.T, energy[:, 0]

    return jax.shard_map(local_run, mesh=mesh, in_specs=(P('data', None), P('data'), P(None, 'parts'), P(None, 'parts')),
                         out_specs=(P(None, 'parts'), P(None, 'parts'), P('parts')), check_vma=False)
```
